32 devices in a mesh: pts: 32 (over z, y, x, core).
Axes of the slice: x: 2, y: 2, z: 4, core: 2. Of those that a mesh axis runs over, the one named last changes fastest.
Arguments:
- point_data: float32 [5, 32768], P(None, 'pts'), may hold values from -1 to 1
- point_counts: int32 [32], P('pts'), may hold values from 64 to 1024, as said below
- point_offsets: int32 [32], P('pts'), may hold values from 0 to 960, as said below
- in_weight: float32 [3, 256], replicated, may hold values from -6 to 6
- input_bias: float32 [256], replicated, may hold values from -3 to 3
- hidden_layer_weight: float32 [3, 256, 256], replicated, may hold values from -0.5 to 0.5
- hidden_bias: float32 [3, 256], replicated, may hold values from -3 to 3
- output_weight: float32 [3, 256], replicated, may hold values from -0.75 to 0.75
- out_bias: float32 [3], replicated, may hold values from -3 to 3
Outputs:
- grad_in_weight: float32 [3, 256], replicated
- grad_in_bias: float32 [256], replicated
- grad_hidden_weight: float32 [3, 256, 256], replicated
- grad_hidden_bias: float32 [3, 256], replicated
- grad_out_weight: float32 [3, 256], replicated
- grad_out_bias: float32 [3], replicated
- term_means: float32 [3], replicated
The draws below stay inside these ranges and needn't reach their ends.
Inputs may be any that keep to these rules, and one draw needn't show every extreme that they name: `point_counts`: some device has exactly 1024 live points and another exactly 64. A device's live points fill its slots point_offsets to point_offsets + point_counts - 1, all within its 1024 slots.
All inputs are finite; a program needn't handle non-finite values.
Results may differ from the reference program's by a relative error of at most 0.0001.
Values sent between devices are 32-bit elements; how exact they have to be, the bound alone decides.
A program may use at most 64 MiB of HBM per device.

```python
import jax
import jax.numpy as jnp
from jax import lax

WIDTH = 256
HID = 3
CAP = 1024
BLOCK = 256
POINTS = 32768


def shared_layout(key):
    devices = POINTS // CAP
    base = jax.random.randint(jax.random.fold_in(key, 11), (devices,), CAP // 16, CAP + 1)
    fullest = jax.random.randint(jax.random.fold_in(key, 12), (), 0, devices)
    sparsest = (fullest + 1 + jax.random.randint(jax.random.fold_in(key, 14), (), 0, devices - 1)) % devices
    index = jnp.arange(devices)
    counts = jnp.where(index == fullest, CAP, jnp.where(index == sparsest, CAP // 16, base)).astype(jnp.int32)
    offsets = jax.random.randint(jax.random.fold_in(key, 13), (devices,), 0, CAP - counts + 1)
    offsets = jnp.where(index == sparsest, CAP - CAP // 16, offsets).astype(jnp.int32)
    return (counts, offsets)


def draw_point_counts(key, part):
    return shared_layout(key)[0]


def draw_point_offsets(key, part):
    return shared_layout(key)[1]


def levels(rng, dims, split, smallest, top_value):
    gain = 1.0
    for axis_at, blocks in split:
        steps = jax.random.uniform(jax.random.fold_in(jax.random.fold_in(rng, 6), axis_at), (blocks,), jnp.float32, smallest / len(split), top_value / len(split))
        gain = gain * jnp.repeat(jnp.exp(steps), dims[axis_at] // blocks).reshape((-1,) + (1,) * (len(dims) - 1 - axis_at))
    return gain


def normal_values(rng, extent, width, reach, kind=jnp.bfloat16):
    return jnp.clip(width * jax.random.normal(rng, extent, jnp.float32), -reach, reach).astype(kind)


def setup_inputs(seed: int = 0) -> dict:
    splits = jax.random.split(jax.random.key(seed), 10)
    return {
        "point_data": jnp.clip(jax.random.uniform(splits[0], (5, POINTS), jnp.float32, -1.0, 1.0) * levels(splits[0], (5, POINTS), ((1, 32),), -0.4, 0.0), -1.0, 1.0),
        "point_counts": draw_point_counts(jax.random.fold_in(splits[9], 71), 0),
        "point_offsets": draw_point_offsets(jax.random.fold_in(splits[9], 71), 0),
        "in_weight": normal_values(splits[3], (3, WIDTH), 1 ** -0.5, 6.0, jnp.float32),
        "input_bias": normal_values(splits[4], (WIDTH,), 0.5, 3.0, jnp.float32),
        "hidden_layer_weight": normal_values(splits[5], (HID, WIDTH, WIDTH), (WIDTH // 2) ** -0.5, 0.5, jnp.float32),
        "hidden_bias": normal_values(splits[6], (HID, WIDTH), 0.3, 3.0, jnp.float32),
        "output_weight": normal_values(splits[7], (3, WIDTH), (WIDTH // 4) ** -0.5, 0.75, jnp.float32),
        "out_bias": normal_values(splits[8], (3,), 0.5, 3.0, jnp.float32),
    }


viscosity = 0.2
term_weights = (2.0, 1.0, 1.0)
highest_precision = lax.Precision.HIGHEST

def apply_tanh(stack_arrays):
    hidden = jnp.tanh(stack_arrays[0])
    slope = 1.0 - hidden * hidden
    firsts = slope[None] * stack_arrays[1:4]
    seconds = slope[None] * stack_arrays[4:6] - 2.0 * (hidden * slope)[None] * stack_arrays[1:3] * stack_arrays[1:3]
    return jnp.concatenate([hidden[None], firsts, seconds], 0)

def add_bias(stack_arrays, bias):
    return jnp.concatenate([stack_arrays[0:1] + bias[None, :, None], stack_arrays[1:]], 0)

def network_jets(params, coords):
    in_weight, input_bias, hidden_layer_weight, hidden_bias, output_weight, out_bias = params
    rows = coords.shape[1]
    value = jnp.dot(in_weight.T, coords, precision=highest_precision, preferred_element_type=jnp.float32) + input_bias[:, None]
    firsts = in_weight[:, :, None] * jnp.ones((1, 1, rows), jnp.float32)
    zeros = jnp.zeros((2,) + value.shape, jnp.float32)
    stack_arrays = jnp.concatenate([value[None], firsts, zeros], 0)
    for layer_apply in range(hidden_layer_weight.shape[0]):
        stack_arrays = jnp.einsum('hm,xmj->xhj', hidden_layer_weight[layer_apply], apply_tanh(stack_arrays), precision=highest_precision)
        stack_arrays = add_bias(stack_arrays, hidden_bias[layer_apply])
    stack_arrays = jnp.einsum('hm,xmj->xhj', output_weight, apply_tanh(stack_arrays), precision=highest_precision)
    return add_bias(stack_arrays, out_bias)

def residual_totals(params, block_data, mask):
    out = network_jets(params, block_data[0:3])
    x_vel, y_vel = (out[0, 0], out[0, 1])
    continuity = out[1, 0] + out[2, 1]
    momentum_x = out[3, 0] + x_vel * out[1, 0] + y_vel * out[2, 0] + out[1, 2] - viscosity * (out[4, 0] + out[5, 0]) - block_data[3]
    momentum_y = out[3, 1] + x_vel * out[1, 1] + y_vel * out[2, 1] + out[2, 2] - viscosity * (out[4, 1] + out[5, 1]) - block_data[4]
    return jnp.stack([jnp.sum(mask * continuity * continuity), jnp.sum(mask * momentum_x * momentum_x), jnp.sum(mask * momentum_y * momentum_y)])

def reference(point_data, point_counts, point_offsets, in_weight, input_bias, hidden_layer_weight, hidden_bias, output_weight, out_bias):
    params = (in_weight, input_bias, hidden_layer_weight, hidden_bias, output_weight, out_bias)
    slots = jnp.arange(POINTS, dtype=jnp.int32)
    local_slot = slots % CAP
    owner = slots // CAP
    first = point_offsets[owner]
    live = ((local_slot >= first) & (local_slot < first + point_counts[owner])).astype(jnp.float32)
    blocks = POINTS // BLOCK
    data_blocks = jnp.transpose(point_data.reshape(5, blocks, BLOCK), (1, 0, 2))
    mask_blocks = live.reshape(blocks, BLOCK)
    weights = jnp.array(term_weights, jnp.float32)

    def step(carry, inputs):
        sums, grads = carry
        block_data, mask = inputs
        block_sums, pullback = jax.vjp(lambda p: residual_totals(p, block_data, mask), params)
        block_grads = pullback(weights)[0]
        return ((sums + block_sums, jax.tree.map(jnp.add, grads, block_grads)), None)
    start = (jnp.zeros((3,), jnp.float32), jax.tree.map(jnp.zeros_like, params))
    (sums, grads), _ = lax.scan(step, start, (data_blocks, mask_blocks))
    total = jnp.sum(point_counts).astype(jnp.float32)
    return (grads[0] / total, grads[1] / total, grads[2] / total, grads[3] / total, grads[4] / total, grads[5] / total, sums / total)
```

```python
import functools

import jax
import jax.numpy as jnp
from jax import lax
from jax.experimental import pallas as pl
from jax.experimental.pallas import tpu as pltpu
from jax.sharding import PartitionSpec as P

viscosity = 0.2
term_weights = (2.0, 1.0, 1.0)
twice = 2.0 * viscosity
B = 256
R = 16

bf16, f32 = jnp.bfloat16, jnp.float32


def split(x):
    hi = x.astype(bf16)
    return hi, (x - hi.astype(f32)).astype(bf16)


def nn(a, b):
    return lax.dot_general(a, b, (((1,), (0,)), ((), ())), preferred_element_type=f32)


def nt(a, b):
    return lax.dot_general(a, b, (((1,), (1,)), ((), ())), preferred_element_type=f32)


def row_sums(x):
    ones = jnp.ones((8, x.shape[1]), f32)
    return lax.dot_general(
        ones,
        x,
        (((1,), (1,)), ((), ())),
        precision=lax.Precision.HIGHEST,
        preferred_element_type=f32,
    )


def local_kernel(
    width,
    hid,
    count_ref,
    offset_ref,
    data_ref,
    in_ref,
    inb_ref,
    w_ref,
    hb_ref,
    wo_ref,
    bo_ref,
    out_ref,
    wcat,
    wtcat,
    wocat,
    wotcat,
    cols,
    z_ref,
    a_ref,
    dz_ref,
    da_ref,
    dout_ref,
    vec,
    tall,
):
    H = width
    for l in range(hid):
        hi, lo = split(w_ref[l])
        wcat[l, :, 0:H] = hi
        wcat[l, :, H : 2 * H] = lo
        wcat[l, :, 2 * H : 3 * H] = hi
        hi, lo = split(w_ref[l].T)
        wtcat[l, :, 0:H] = hi
        wtcat[l, :, H : 2 * H] = lo
        wtcat[l, :, 2 * H : 3 * H] = hi
    tall[...] = jnp.zeros_like(tall)
    tall[0:3, :] = in_ref[...]
    tall[3:4, :] = inb_ref[...]
    tall[4 : 4 + hid, :] = hb_ref[...]
    cols[...] = tall[...].T
    tall[...] = jnp.zeros_like(tall)
    tall[0:3, :] = wo_ref[...]
    hi, lo = split(tall[0:16, :])
    wocat[:, 0:H] = hi
    wocat[:, H : 2 * H] = lo
    wocat[:, 2 * H : 3 * H] = hi
    tall[0:16, :] = hi.astype(f32)
    tall[16:32, :] = lo.astype(f32)
    tall[32:48, :] = hi.astype(f32)
    wotcat[...] = tall[...].T.astype(bf16)
    tall[...] = jnp.zeros_like(tall)
    vec[...] = jnp.zeros_like(vec)
    out_ref[...] = jnp.zeros_like(out_ref)
    dout_ref[...] = jnp.zeros_like(dout_ref)

    count = count_ref[0]
    start = offset_ref[0]
    first = start // B
    end = (start + count + B - 1) // B

    def put_jets(ref, rows, jets, l=None):
        for j, v in enumerate(jets):
            hi, lo = split(v)
            lanes = slice(j * B, (j + 1) * B)
            for k, part in enumerate((hi, hi, lo)):
                at = slice(k * H + rows, k * H + rows + R)
                if l is None:
                    ref[at, lanes] = part
                else:
                    ref[l, at, lanes] = part

    def column(k, rows):
        return jnp.broadcast_to(cols[rows : rows + R, k : k + 1], (R, B))

    def tanh_jets(a, zx, zy, zt):
        s = 1.0 - a * a
        q = zx * zx + zy * zy
        return a, s * zx, s * zy, s * (zt + (twice * a) * q)

    def half(v):
        return v[:, 0 : B // 2] + v[:, B // 2 : B]

    def tanh_back(a, zx, zy, zt, da, dax, day, dat):
        s = 1.0 - a * a
        q = zx * zx + zy * zy
        ca = twice * a
        ds = dax * zx + day * zy + dat * (zt + ca * q)
        dz = s * (da + (twice * dat) * (s * q) - 2.0 * (a * ds))
        e = 2.0 * (ca * dat)
        return dz, s * (dax + e * zx), s * (day + e * zy), s * dat

    def step(index, carry):
        lanes = pl.ds(pl.multiple_of(index * B, B), B)
        x = data_ref[0:1, lanes]
        y = data_ref[1:2, lanes]
        t = data_ref[2:3, lanes]
        fx = data_ref[3:4, lanes]
        fy = data_ref[4:5, lanes]
        slots = index * B + lax.broadcasted_iota(jnp.int32, (1, B), 1)
        mask = ((slots >= start) & (slots < start + count)).astype(f32)
        for r in range(0, H, R):
            wx, wy, wt = column(0, r), column(1, r), column(2, r)
            a = jnp.tanh(wx * x + wy * y + wt * t + column(3, r))
            z_ref[0, r : r + R, 0:B] = a
            put_jets(a_ref, r, tanh_jets(a, wx, wy, wt), 0)
        for l in range(hid):
            z_ref[l + 1] = nn(wcat[l], a_ref[l])
            for r in range(0, H, R):
                rows = slice(r, r + R)
                a = jnp.tanh(z_ref[l + 1, rows, 0:B] + column(4 + l, r))
                z_ref[l + 1, rows, 0:B] = a
                zx, zy, zt = (z_ref[l + 1, rows, j * B : (j + 1) * B] for j in (1, 2, 3))
                put_jets(a_ref, r, tanh_jets(a, zx, zy, zt), l + 1)
        out = nn(wocat[...], a_ref[hid])
        u = out[0:1, 0:B] + bo_ref[0]
        v = out[1:2, 0:B] + bo_ref[1]
        ux, vx, px = (out[k : k + 1, B : 2 * B] for k in range(3))
        uy, vy, py = (out[k : k + 1, 2 * B : 3 * B] for k in range(3))
        ut, vt = (out[k : k + 1, 3 * B : 4 * B] for k in range(2))
        c = mask * (ux + vy)
        mx = mask * (ut + u * ux + v * uy + px - fx)
        my = mask * (vt + u * vx + v * vy + py - fy)
        rc = (2.0 * term_weights[0]) * c
        rx = (2.0 * term_weights[1]) * mx
        ry = (2.0 * term_weights[2]) * my
        du = rx * ux + ry * vx
        dv = rx * uy + ry * vy
        row = lax.broadcasted_iota(jnp.int32, (R, B), 0)
        zero = jnp.zeros((1, B), f32)

        def three(p0, p1, p2):
            return jnp.where(
                row == 0, p0, jnp.where(row == 1, p1, jnp.where(row == 2, p2, 0.0))
            )

        tall[0:16, :] += jnp.where(row < 3, three(c * c, mx * mx, my * my), 0.0) + jnp.where(
            row == 3, du, jnp.where(row == 4, dv, 0.0)
        )
        douts = (
            three(du, dv, zero),
            three(rc + rx * u, ry * u, rx),
            three(rx * v, rc + ry * v, ry),
            three(rx, ry, zero),
        )
        for j, d in enumerate(douts):
            hi, lo = split(d)
            at = slice(j * B, (j + 1) * B)
            dout_ref[0:16, at] = hi
            dout_ref[16:32, at] = hi
            dout_ref[32:48, at] = lo
        both = nt(dout_ref[16:48, :], a_ref[hid, 0:H, :])
        both = both[0:16] + both[16:32] + nt(dout_ref[0:16, :], a_ref[hid, 2 * H : 3 * H, :])
        out_ref[hid * H + 8 : hid * H + 16, :] += both[0:8]
        da_ref[...] = nn(wotcat[...], dout_ref[...])
        for l in range(hid, 0, -1):
            for r in range(0, H, R):
                rows = slice(r, r + R)
                a, zx, zy, zt = (z_ref[l, rows, j * B : (j + 1) * B] for j in range(4))
                ds = (da_ref[rows, j * B : (j + 1) * B] for j in range(4))
                dz = tanh_back(a, zx, zy, zt, *ds)
                put_jets(dz_ref, r, dz)
                vec[3 + l, rows, :] += half(dz[0])
            da_ref[...] = nn(wtcat[l - 1], dz_ref[...])
            both = nt(dz_ref[H : 3 * H, :], a_ref[l - 1, 0:H, :])
            both = both[0:H] + both[H : 2 * H]
            both = both + nt(dz_ref[0:H, :], a_ref[l - 1, 2 * H : 3 * H, :])
            out_ref[(l - 1) * H : l * H, :] += both
        for r in range(0, H, R):
            rows = slice(r, r + R)
            a = z_ref[0, rows, 0:B]
            ds = (da_ref[rows, j * B : (j + 1) * B] for j in range(4))
            dz, dzx, dzy, dzt = tanh_back(a, column(0, r), column(1, r), column(2, r), *ds)
            vec[0, rows, :] += half(dz * x + dzx)
            vec[1, rows, :] += half(dz * y + dzy)
            vec[2, rows, :] += half(dz * t + dzt)
            vec[3, rows, :] += half(dz)
        return carry

    lax.fori_loop(first, end, step, 0)
    base = hid * H
    for k in range(4 + hid):
        out_ref[base + k : base + k + 1, :] = row_sums(vec[k])[0:1]
    lane = lax.broadcasted_iota(jnp.int32, (1, tall.shape[0]), 1)
    scalars = row_sums(tall[...])[0:1] + jnp.where(lane == 6, count.astype(f32), 0.0)
    out_ref[base + 7 : base + 8, 0 : tall.shape[0]] = scalars


def local_terms(counts, offsets, data, in_w, in_b, w, hb, wo, bo):
    hid, H, _ = w.shape
    vm = pl.BlockSpec(memory_space=pltpu.VMEM)
    sm = pl.BlockSpec(memory_space=pltpu.SMEM)
    return pl.pallas_call(
        functools.partial(local_kernel, H, hid),
        out_shape=jax.ShapeDtypeStruct((hid * H + 16, H), f32),
        in_specs=[sm, sm, vm, vm, vm, vm, vm, vm, sm],
        out_specs=vm,
        scratch_shapes=[
            pltpu.VMEM((hid, H, 3 * H), bf16),
            pltpu.VMEM((hid, H, 3 * H), bf16),
            pltpu.VMEM((16, 3 * H), bf16),
            pltpu.VMEM((H, 128), bf16),
            pltpu.VMEM((H, 128), f32),
            pltpu.VMEM((hid + 1, H, 4 * B), f32),
            pltpu.VMEM((hid + 1, 3 * H, 4 * B), bf16),
            pltpu.VMEM((3 * H, 4 * B), bf16),
            pltpu.VMEM((H, 4 * B), f32),
            pltpu.VMEM((128, 4 * B), bf16),
            pltpu.VMEM((4 + hid, H, 128), f32),
            pltpu.VMEM((128, H), f32),
        ],
        compiler_params=pltpu.CompilerParams(vmem_limit_bytes=56 * 1024 * 1024),
        name="local_terms",
    )(counts, offsets, data, in_w, in_b.reshape(1, H), w, hb, wo, bo)


MESH = pl.DeviceIdType.MESH

def stages_of(n, rows):
    out, stride = [], 1
    radices = []
    left = n
    if left % 2 == 0:
        radices.append(2); left //= 2
    while left % 4 == 0:
        radices.append(4); left //= 4
    if left > 1:
        radices.append(left)
    for r in radices:
        scatter = rows % (8 * r) == 0
        if scatter:
            rows //= r
        out.append((stride, r, rows, scatter))
        stride *= r
    return out

def ar_kernel(n, hid, H, stages, order, x_ref, w_ref, gi_ref, gb_ref, gh_ref, go_ref, gob_ref, terms_ref, *scratch):
    ns = len(stages)
    bufs = scratch[:ns]
    accs = scratch[ns:2 * ns]
    sbufs = scratch[2 * ns:3 * ns]
    saccs = scratch[3 * ns]
    send, recv, gsend, grecv, ssend, srecv = scratch[3 * ns + 1:]
    me = lax.axis_index("pts")
    peers, digit = [], []
    for stride, r, rows, sc in stages:
        d = (me // stride) % r
        digit.append(d)
        peers.append([me + ((d + k) % r - d) * stride for k in range(1, r)])
    barrier = pltpu.get_barrier_semaphore()
    cnt = 0
    for ps in peers:
        for p in ps:
            pl.semaphore_signal(barrier, inc=1, device_id=(p,), device_id_type=MESH)
            cnt += 1
    pl.semaphore_wait(barrier, cnt)
    hid_rows = hid * H

    def small_src(s):
        return x_ref.at[hid_rows:hid_rows + 16, :] if s == 0 else saccs.at[s - 1]

    def small_start(s):
        cs = []
        for k, p in enumerate(peers[s]):
            c = pltpu.make_async_remote_copy(small_src(s), sbufs[s].at[k], ssend.at[s, k], srecv.at[s, k], device_id=(p,), device_id_type=MESH)
            c.start(); cs.append(c)
        return cs

    def small_finish(s, cs):
        for c in cs:
            c.wait()
        v = small_src(s)[...]
        for k in range(len(cs)):
            v = v + sbufs[s][k]
        saccs[s] = v

    def src_rows(l, s, at, rows):
        if s == 0:
            return x_ref.at[pl.ds(pl.multiple_of(l * H + at, 8), rows), :]
        return accs[s - 1].at[l, pl.ds(pl.multiple_of(at, 8), rows), :]

    def start(l, s):
        stride, r, rows, sc = stages[s]
        cs = []
        for k, p in enumerate(peers[s]):
            at = ((digit[s] + k + 1) % r) * rows if sc else 0
            c = pltpu.make_async_remote_copy(src_rows(l, s, at, rows), bufs[s].at[l, k], send.at[l, s, k], recv.at[l, s, k], device_id=(p,), device_id_type=MESH)
            c.start(); cs.append(c)
        return cs

    def finish(l, s, cs, scale=None):
        stride, r, rows, sc = stages[s]
        for c in cs:
            c.wait()
        v = src_rows(l, s, digit[s] * rows if sc else 0, rows)[...]
        for k in range(r - 1):
            v = v + bufs[s][l, k]
        if scale is not None:
            w_ref[l, pl.ds(pl.multiple_of(base[s], 8), rows), :] = v * scale
        else:
            accs[s][l] = v

    base, b = [], 0
    for s, (stride, r, rows, sc) in enumerate(stages):
        if sc:
            b = b + digit[s] * rows
        base.append(b)

    def gstart(l, s):
        stride, r, rows, sc = stages[s]
        if not sc:
            return []
        at = pl.ds(pl.multiple_of(base[s], 8), rows)
        cs = []
        for k, p in enumerate(peers[s]):
            c = pltpu.make_async_remote_copy(w_ref.at[l, at, :], w_ref.at[l, at, :], gsend.at[l, s, k], grecv.at[l, s, k], device_id=(p,), device_id_type=MESH)
            c.start(); cs.append(c)
        return cs

    flight = {}
    sf = small_start(0)
    for l in order:
        flight[l] = start(l, 0)
    for s in range(ns):
        small_finish(s, sf)
        if s + 1 < ns:
            sf = small_start(s + 1)
        else:
            inv = 1.0 / saccs[ns - 1, 7:8, 6:7]
            small = saccs[ns - 1] * inv
            gi_ref[...] = small[0:3]
            gb_ref[...] = small[3:4]
            gh_ref[...] = small[4 : 4 + hid]
            go_ref[...] = small[8:11]
            for k in range(3):
                terms_ref[k] = small[7, k]
                gob_ref[k] = small[7, 3 + k]
        for l in order:
            finish(l, s, flight[l], None if s + 1 < ns else inv)
            flight[l] = start(l, s + 1) if s + 1 < ns else gstart(l, ns - 1)
    for s in range(ns - 1, -1, -1):
        for l in order:
            for c in flight[l]:
                c.wait()
            flight[l] = gstart(l, s - 1) if s > 0 else []

def all_reduce(x, n, hid, H, order=None, cid=0):
    stages = stages_of(n, H)
    ns = len(stages)
    kmax = max(r for _, r, _, _ in stages) - 1
    order = order or tuple(range(hid - 1, -1, -1))
    vm = pl.BlockSpec(memory_space=pltpu.VMEM)
    sm = pl.BlockSpec(memory_space=pltpu.SMEM)
    DMA = pltpu.SemaphoreType.DMA
    return pl.pallas_call(
        functools.partial(ar_kernel, n, hid, H, stages, order),
        out_shape=tuple(jax.ShapeDtypeStruct(k, f32) for k in ((hid, H, H), (3, H), (1, H), (hid, H), (3, H), (3,), (3,))),
        in_specs=[vm],
        out_specs=(vm, vm, vm, vm, vm, sm, sm),
        scratch_shapes=[pltpu.VMEM((hid, r - 1, rows, H), f32) for _, r, rows, _ in stages]
        + [pltpu.VMEM((hid, rows, H), f32) for _, r, rows, _ in stages]
        + [pltpu.VMEM((r - 1, 16, H), f32) for _, r, rows, _ in stages]
        + [pltpu.VMEM((ns, 16, H), f32)]
        + [DMA((hid, ns, kmax)), DMA((hid, ns, kmax)), DMA((hid, ns, kmax)), DMA((hid, ns, kmax)), DMA((ns, kmax)), DMA((ns, kmax))],
        compiler_params=pltpu.CompilerParams(collective_id=cid, has_side_effects=True, vmem_limit_bytes=32 * 1024 * 1024),
        name="all_reduce",
    )(x)


def shards(n, data, counts, offsets, in_w, in_b, w, hb, wo, bo):
    hid, H, _ = w.shape
    mine = local_terms(counts, offsets, data, in_w, in_b, w, hb, wo, bo)
    gw, gi, gb, gh, go, gob, terms = all_reduce(mine, n, hid, H)
    return gi, gb.reshape(H), gw, gh, go, gob, terms


def solution(mesh):
    placed = (P(None, "pts"), P("pts"), P("pts"), P(), P(), P(), P(), P(), P())
    return jax.shard_map(
        functools.partial(shards, mesh.shape["pts"]),
        mesh=mesh,
        in_specs=placed,
        out_specs=(P(), P(), P(), P(), P(), P(), P()),
        check_vma=False,
    )
```
